32 devices in a mesh: group: 16 (over z, y, core), helper: 2 (over x).
Axes of the slice: x: 2, y: 2, z: 4, core: 2. Of those that a mesh axis runs over, the one named last changes fastest.
Arguments:
- candidates: bfloat16 [16, 512, 1024], P('group', 'helper'), may hold values from -6 to 6
- prefix_cache: bfloat16 [16, 2, 768, 1024], P('group', None, 'helper'), may hold values from -6 to 6
- w_uvqk: bfloat16 [1024, 4096], replicated, may hold values from -0.1875 to 0.1875
- w_output: bfloat16 [1024, 1024], replicated, may hold values from -0.1875 to 0.1875
- norm_gain: float32 [1024], replicated, may hold values from 0.1 to 1.9
- owner: int32 [16], replicated, may hold values from 0 to 15, as said below
- counts: int32 [16], replicated, may hold values from 256 to 512, as said below
- prefix_len: int32 [16], replicated, may hold values from 24 to 768, as said below
Outputs:
- update: bfloat16 [16, 512, 1024], P('group', 'helper')
The draws below stay inside these ranges and needn't reach their ends.
Inputs may be any that keep to these rules, and one draw needn't show every extreme that they name: owner[u] = (u + s) mod 16 for one shift s of the round. `counts`: multiples of 128; some user has exactly 512. `prefix_len`: some user has exactly 768.
All inputs are finite; a program needn't handle non-finite values.
Results may differ from the reference program's by a relative error of at most 0.012.
Values may be sent and summed in bfloat16 or wider, within the bound.
A program may use at most 128 MiB of HBM per device.

```python
import jax
import jax.numpy as jnp
from jax import lax

D = 1024
HEADS = 8
PREFIX = 768
CAND = 512
GRAIN = 128
USERS = 16


def draw_owner(key, part):
    offset = jax.random.randint(key, (), 0, USERS)
    return ((jnp.arange(USERS, dtype=jnp.int32) + offset) % USERS).astype(jnp.int32)


def draw_counts(key, part):
    first, second = jax.random.split(jax.random.fold_in(key, 11))
    steps = jax.random.randint(first, (USERS,), CAND // (2 * GRAIN), CAND // GRAIN + 1)
    chosen = jax.random.randint(second, (), 0, USERS)
    values = jnp.where(jnp.arange(USERS) == chosen, CAND, steps * GRAIN)
    return values.astype(jnp.int32)


def draw_prefix_len(key, part):
    first, second = jax.random.split(jax.random.fold_in(key, 23))
    values = jax.random.randint(first, (USERS,), max(1, PREFIX // 32), PREFIX + 1)
    chosen = jax.random.randint(second, (), 0, USERS)
    values = jnp.where(jnp.arange(USERS) == chosen, PREFIX, values)
    return values.astype(jnp.int32)


def block_levels(own_key, dims, shards, smallest, high):
    def one(position, blocks):
        draws = jax.random.uniform(jax.random.fold_in(jax.random.fold_in(own_key, 6), position), (blocks,), jnp.float32, smallest / len(shards), high / len(shards))
        return jnp.repeat(jnp.exp(draws), dims[position] // blocks).reshape((-1,) + (1,) * (len(dims) - position - 1))

    factor_of = one(*shards[0])
    for cut in shards[1:]:
        factor_of = factor_of * one(*cut)
    return factor_of


def noise(stream_key, shape, scale, most, cuts=(), kind=jnp.bfloat16):
    level = block_levels(stream_key, shape, cuts, -0.22, 0.18) if cuts else 1.0
    values = jax.random.normal(stream_key, shape, jnp.float32) * scale * level
    return jnp.minimum(jnp.maximum(values, -most), most).astype(kind)


def setup_inputs(seed: int = 0) -> dict:
    seeds = jax.random.split(jax.random.key(seed), 9)
    candidates = noise(seeds[0], (USERS, CAND, D), 1.0, 6.0, ((0, 16), (1, 2)))
    prefix_cache = noise(seeds[1], (USERS, 2, PREFIX, D), 1.0, 6.0, ((0, 16), (2, 2)))
    w_uvqk = noise(seeds[2], (D, 4 * D), D ** -0.5, 0.1875)
    w_output = noise(seeds[3], (D, D), D ** -0.5, 0.1875)
    norm_gain = jnp.clip(1.0 + 0.18 * jax.random.normal(seeds[4], (D,), jnp.float32), 0.1, 1.9)
    owner = draw_owner(jax.random.fold_in(seeds[8], 71), 0)
    counts = draw_counts(jax.random.fold_in(seeds[8], 71), 0)
    prefix_len = draw_prefix_len(jax.random.fold_in(seeds[8], 71), 0)
    return dict(candidates=candidates, prefix_cache=prefix_cache, w_uvqk=w_uvqk, w_output=w_output, norm_gain=norm_gain, owner=owner, counts=counts, prefix_len=prefix_len)


def score_user(rows, keys, values, count, visible, w_uvqk, w_output, norm_gain):
    width = rows.shape[1]
    head = width // HEADS
    scale = head ** (-0.5)
    total = rows.shape[0]
    proj = jax.nn.silu(jnp.dot(rows, w_uvqk, preferred_element_type=jnp.float32))
    gate_u = proj[:, :width]
    own_v = proj[:, width:2 * width].astype(jnp.bfloat16).astype(jnp.float32).reshape(total, HEADS, head)
    query = proj[:, 2 * width:3 * width].astype(jnp.bfloat16).astype(jnp.float32).reshape(total, HEADS, head)
    own_k = proj[:, 3 * width:].astype(jnp.bfloat16).astype(jnp.float32).reshape(total, HEADS, head)
    length = keys.shape[0]
    keys4 = keys.astype(jnp.float32).reshape(length, HEADS, head)
    values4 = values.astype(jnp.float32).reshape(length, HEADS, head)
    scores = jnp.einsum('rhd,nhd->hrn', query, keys4) * scale
    allowed = jnp.arange(length, dtype=jnp.int32) < visible
    weights = jnp.where(allowed[None, None, :], jax.nn.silu(scores), 0.0).astype(jnp.bfloat16).astype(jnp.float32)
    mixed = jnp.einsum('hrn,nhd->rhd', weights, values4)
    selfw = jax.nn.silu(lax.optimization_barrier(jnp.sum(query * own_k, axis=-1)) * scale).astype(jnp.bfloat16).astype(jnp.float32)
    mixed = (mixed + selfw[:, :, None] * own_v).reshape(total, width)
    centre = mixed - lax.optimization_barrier(jnp.mean(mixed, axis=-1, keepdims=True))
    spread = lax.optimization_barrier(jnp.mean(centre * centre, axis=-1, keepdims=True))
    normed = (centre * lax.rsqrt(spread + 1e-05) * norm_gain * gate_u).astype(jnp.bfloat16)
    result = jnp.dot(normed, w_output, preferred_element_type=jnp.float32)
    live = jnp.arange(total, dtype=jnp.int32) < count
    return jnp.where(live[:, None], result, 0.0).astype(jnp.bfloat16)

def reference(candidates, prefix_cache, w_uvqk, w_output, norm_gain, owner, counts, prefix_len):
    shift = owner[0]

    def one_user(user):
        rows = lax.dynamic_index_in_dim(candidates, user, 0, keepdims=False)
        source = ((user + shift) % USERS).astype(jnp.int32)
        cache = lax.dynamic_index_in_dim(prefix_cache, source, 0, keepdims=False)
        count = lax.dynamic_index_in_dim(counts, user, 0, keepdims=False)
        visible = lax.dynamic_index_in_dim(prefix_len, user, 0, keepdims=False)
        return score_user(rows, cache[0], cache[1], count, visible, w_uvqk, w_output, norm_gain)
    result = lax.map(one_user, jnp.arange(USERS, dtype=jnp.int32))
    return jnp.roll(result, shift, axis=0)
```

```python
import functools
import math

import jax
import jax.numpy as jnp
from jax import lax
from jax.experimental import pallas as pl
from jax.experimental.pallas import tpu as pltpu
from jax.sharding import PartitionSpec as P

HEADS = 8
EPS = 1e-05


def pick(table, index):
    places = jnp.arange(table.shape[0], dtype=jnp.int32)
    return jnp.sum(jnp.where(places == index, table, 0))


def silu(v):
    t = v * 0.5
    return t + t * jnp.tanh(t)


def attend(query, keys, values, scale):
    scores = lax.dot_general(
        query, keys, (((1,), (1,)), ((), ())), preferred_element_type=jnp.float32
    )
    t = scores * (0.5 * scale)
    weights = (t + t * jnp.tanh(t)).astype(jnp.bfloat16)
    return jnp.dot(weights, values, preferred_element_type=jnp.float32)


def seen(values, base, visible):
    rows = lax.broadcasted_iota(jnp.int32, values.shape, 0) + base
    return jnp.where(rows < visible, values, jnp.zeros_like(values))


def first_kernel(head, scale, info, tok, wu, wv, wq, wk, kref, vref, u_out, q_out, acc_out):
    tokens = tok[...]
    u_out[...] = silu(jnp.dot(tokens, wu[...], preferred_element_type=jnp.float32))
    own_v = silu(jnp.dot(tokens, wv[...], preferred_element_type=jnp.float32)).astype(jnp.bfloat16)
    query = silu(jnp.dot(tokens, wq[...], preferred_element_type=jnp.float32)).astype(jnp.bfloat16)
    own_k = silu(jnp.dot(tokens, wk[...], preferred_element_type=jnp.float32)).astype(jnp.bfloat16)
    q_out[...] = query
    prod = query.astype(jnp.float32) * own_k.astype(jnp.float32)
    own_v = own_v.astype(jnp.float32)
    values = seen(vref[...], info[2], info[0])
    for n in range(query.shape[1] // head):
        cols = slice(n * head, (n + 1) * head)
        selfw = silu(jnp.sum(prod[:, cols], axis=1, keepdims=True) * scale)
        selfw = selfw.astype(jnp.bfloat16).astype(jnp.float32)
        mixed = attend(query[:, cols], kref[:, cols], values[:, cols], scale)
        acc_out[:, cols] = mixed + selfw * own_v[:, cols]


def last_kernel(head, scale, pieces, info, q, acc, u, gain, w_out, *rest):
    kvs, out, total = rest[: 2 * pieces], rest[2 * pieces], rest[2 * pieces + 1]
    step = pl.program_id(0)
    wide = q.shape[1]
    mixed = [acc[:, n * head : (n + 1) * head] for n in range(wide // head)]
    for p in range(pieces):
        kref, vref = kvs[2 * p], kvs[2 * p + 1]
        values = seen(vref[...], info[3 + p], info[0])
        for n in range(wide // head):
            cols = slice(n * head, (n + 1) * head)
            mixed[n] += attend(q[:, cols], kref[:, cols], values[:, cols], scale)
    for n in range(wide // head):
        start = pl.multiple_of(step * wide + n * head, head)
        total[:, pl.ds(start, head)] = mixed[n]

    @pl.when(step == pl.num_programs(0) - 1)
    def _():
        a = total[...]
        centre = a - jnp.mean(a, axis=-1, keepdims=True)
        spread = jnp.mean(centre * centre, axis=-1, keepdims=True)
        normed = (centre * lax.rsqrt(spread + EPS) * gain[...] * u[...]).astype(jnp.bfloat16)
        result = jnp.dot(normed, w_out[...], preferred_element_type=jnp.float32)
        rows = lax.broadcasted_iota(jnp.int32, result.shape, 0)
        out[...] = jnp.where(rows < info[1], result, 0.0).astype(jnp.bfloat16)


def local(candidates, prefix_cache, w_uvqk, w_output, norm_gain, owner, counts, prefix_len):
    groups = lax.axis_size("group")
    helpers = lax.axis_size("helper")
    group_here = lax.axis_index("group")
    helper_here = lax.axis_index("helper")
    offset = owner[0]
    _, slots, width = candidates.shape
    length = prefix_cache.shape[2]
    head = width // HEADS
    scale = head ** (-0.5)
    cache = prefix_cache.reshape(2, length, width)
    got = [
        lax.ppermute(cache, "helper", [(i, (i + j) % helpers) for i in range(helpers)])
        for j in range(1, helpers)
    ]

    def turn(s):
        pairs = [(i, (i + s) % groups) for i in range(groups)]
        return lambda t: lax.ppermute(t, "group", pairs) if s else t

    tokens = lax.switch(offset, [turn(s) for s in range(groups)], candidates[0])
    user = (group_here - offset) % groups
    count = pick(counts, user)
    visible = pick(prefix_len, user)
    live = jnp.clip(count - helper_here * slots, 0, slots)
    bases = [((helper_here - j) % helpers) * length for j in range(helpers)]
    info = jnp.stack([visible, live] + bases).astype(jnp.int32)

    wide = 2 * head
    steps = width // wide
    smem = pl.BlockSpec(memory_space=pltpu.SMEM)
    block = lambda rows: pl.BlockSpec((rows, wide), lambda i: (0, i))
    whole = lambda *shape: pl.BlockSpec(shape, lambda i: (0,) * len(shape))
    part = lambda k: pl.BlockSpec((None, length, wide), lambda i: (k, 0, i))
    weight = lambda k: pl.BlockSpec((width, wide), lambda i: (0, k * steps + i))
    gate_u, query, acc = pl.pallas_call(
        functools.partial(first_kernel, head, scale),
        grid=(steps,),
        in_specs=[smem, whole(slots, width)]
        + [weight(k) for k in range(4)]
        + [part(0), part(1)],
        out_specs=[block(slots)] * 3,
        out_shape=[
            jax.ShapeDtypeStruct((slots, width), jnp.float32),
            jax.ShapeDtypeStruct((slots, width), jnp.bfloat16),
            jax.ShapeDtypeStruct((slots, width), jnp.float32),
        ],
        cost_estimate=pl.CostEstimate(
            flops=2 * slots * width * (4 * width + 2 * length),
            bytes_accessed=8 * width * width + 4 * length * width + 12 * slots * width,
            transcendentals=slots * (4 * width + HEADS * length),
        ),
        compiler_params=pltpu.CompilerParams(dimension_semantics=("arbitrary",)),
        name="first",
    )(info, tokens, w_uvqk, w_uvqk, w_uvqk, w_uvqk, cache, cache)
    pieces = helpers - 1
    result = pl.pallas_call(
        functools.partial(last_kernel, head, scale, pieces),
        grid=(steps,),
        in_specs=[
            smem,
            block(slots),
            block(slots),
            whole(slots, width),
            whole(1, width),
            whole(width, width),
        ]
        + [part(0), part(1)] * pieces,
        out_specs=whole(slots, width),
        out_shape=jax.ShapeDtypeStruct((slots, width), jnp.bfloat16),
        scratch_shapes=[pltpu.VMEM((slots, width), jnp.float32)],
        cost_estimate=pl.CostEstimate(
            flops=2 * slots * width * (width + 2 * length * pieces),
            bytes_accessed=2 * width * width + 4 * length * width * pieces + 12 * slots * width,
            transcendentals=slots * HEADS * length * pieces,
        ),
        compiler_params=pltpu.CompilerParams(dimension_semantics=("arbitrary",)),
        name="last",
    )(info, query, acc, gate_u, norm_gain.reshape(1, width), w_output, *[g for g in got for _ in (0, 1)])
    return result[None]


def solution(mesh):
    in_specs = (
        P("group", "helper", None),
        P("group", None, "helper", None),
        P(),
        P(),
        P(),
        P(),
        P(),
        P(),
    )
    out_specs = P("group", "helper", None)
    return jax.shard_map(local, mesh=mesh, in_specs=in_specs, out_specs=out_specs, check_vma=False)
```

```python
import functools
import math

import jax
import jax.numpy as jnp
from jax import lax
from jax.experimental import pallas as pl
from jax.experimental.pallas import tpu as pltpu
from jax.sharding import PartitionSpec as P

HEADS = 8
EPS = 1e-05


def silu(v):
    t = v * 0.5
    return t + t * jnp.tanh(t)


def weigh(query, keys, scale):
    scores = lax.dot_general(
        query, keys, (((1,), (1,)), ((), ())), preferred_element_type=jnp.float32
    )
    t = scores * (0.5 * scale)
    return (t + t * jnp.tanh(t)).astype(jnp.bfloat16)


def user_here(owner):
    groups = lax.axis_size("group")
    return lax.rem(lax.axis_index("group") - owner[0] + groups, groups)


def piece_base(away, length):
    helpers = lax.axis_size("helper")
    return lax.rem(lax.axis_index("helper") - away + helpers, helpers) * length


def seen(values, base, visible):
    rows = lax.broadcasted_iota(jnp.int32, values.shape, 0) + base
    return jnp.where(rows < visible, values, jnp.zeros_like(values))


def first_kernel(head, scale, owner, prefix_len, tok, w, cache, u_out, q_out, acc_out):
    width = tok.shape[1]
    wide = 2 * head
    length = cache.shape[1]
    visible = prefix_len[user_here(owner)]
    base = piece_base(0, length)
    for pair in range(width // wide):
        cols = slice(pair * wide, (pair + 1) * wide)

        def project(k):
            at = slice(k * width + pair * wide, k * width + (pair + 1) * wide)
            return silu(jnp.dot(tok[...], w[:, at], preferred_element_type=jnp.float32))

        query = project(2).astype(jnp.bfloat16)
        q_out[:, cols] = query
        own_k = project(3).astype(jnp.bfloat16).astype(jnp.float32)
        own_v = project(1).astype(jnp.bfloat16).astype(jnp.float32)
        u_out[:, cols] = project(0)
        prod = query.astype(jnp.float32) * own_k
        values = seen(cache[1, :, cols], base, visible)
        for n in range(wide // head):
            here = slice(n * head, (n + 1) * head)
            at = slice(pair * wide + n * head, pair * wide + (n + 1) * head)
            selfw = silu(jnp.sum(prod[:, here], axis=1, keepdims=True) * scale)
            selfw = selfw.astype(jnp.bfloat16).astype(jnp.float32)
            weights = weigh(query[:, here], cache[0, :, at], scale)
            mixed = jnp.dot(weights, values[:, here], preferred_element_type=jnp.float32)
            acc_out[:, at] = mixed + selfw * own_v[:, here]


def weigh_kernel(head, scale, q, *refs):
    pieces = len(refs) // 2
    for p in range(pieces):
        for n in range(q.shape[1] // head):
            at = slice(n * head, (n + 1) * head)
            refs[pieces + p][n] = weigh(q[:, at], refs[p][:, at], scale)


def last_kernel(head, pieces, owner, counts, prefix_len, acc, u, gain, w_out, *refs):
    weights, values, out, total = refs[:pieces], refs[pieces : 2 * pieces], refs[-2], refs[-1]
    slots, width = acc.shape
    user = user_here(owner)
    visible = prefix_len[user]
    live = counts[user] - lax.axis_index("helper") * slots
    for n in range(width // head):
        at = slice(n * head, (n + 1) * head)
        mixed = acc[:, at]
        for p in range(pieces):
            part = seen(values[p][:, at], piece_base(p + 1, values[p].shape[0]), visible)
            mixed += jnp.dot(weights[p][n], part, preferred_element_type=jnp.float32)
        total[:, at] = mixed
    block = math.gcd(slots, 128)
    for first in range(0, slots, block):
        rows = slice(first, first + block)
        a = total[rows, :]
        centre = a - jnp.mean(a, axis=-1, keepdims=True)
        spread = jnp.mean(centre * centre, axis=-1, keepdims=True)
        normed = (centre * lax.rsqrt(spread + EPS) * gain[...] * u[rows, :]).astype(jnp.bfloat16)
        result = jnp.dot(normed, w_out[...], preferred_element_type=jnp.float32)
        places = lax.broadcasted_iota(jnp.int32, result.shape, 0) + first
        out[rows, :] = jnp.where(places < live, result, 0.0).astype(jnp.bfloat16)


def local(candidates, prefix_cache, w_uvqk, w_output, norm_gain, owner, counts, prefix_len):
    groups = lax.axis_size("group")
    helpers = lax.axis_size("helper")
    _, slots, width = candidates.shape
    length = prefix_cache.shape[2]
    head = width // HEADS
    scale = head ** (-0.5)
    cache = prefix_cache.reshape(2, length, width)
    pieces = helpers - 1

    def from_helper(value, away):
        pairs = [(i, (i + away) % helpers) for i in range(helpers)]
        return lax.ppermute(value, "helper", pairs)

    keys = [from_helper(cache[0], away) for away in range(1, helpers)]
    values = [from_helper(cache[1], away) for away in range(1, helpers)]

    def turn(s):
        pairs = [(i, (i + s) % groups) for i in range(groups)]
        return lambda t: lax.ppermute(t, "group", pairs) if s else t

    tokens = lax.switch(owner[0], [turn(s) for s in range(groups)], candidates[0])

    smem = pl.BlockSpec(memory_space=pltpu.SMEM)
    vmem = pl.BlockSpec(memory_space=pltpu.VMEM)
    params = pltpu.CompilerParams(vmem_limit_bytes=28 * 1024 * 1024)
    rows = lambda kind: jax.ShapeDtypeStruct((slots, width), kind)
    gate_u, query, acc = pl.pallas_call(
        functools.partial(first_kernel, head, scale),
        in_specs=[smem, smem, vmem, vmem, vmem],
        out_specs=[vmem] * 3,
        out_shape=[rows(jnp.float32), rows(jnp.bfloat16), rows(jnp.float32)],
        cost_estimate=pl.CostEstimate(
            flops=2 * slots * width * (4 * width + 2 * length),
            bytes_accessed=8 * width * width + 4 * length * width + 12 * slots * width,
            transcendentals=slots * (4 * width + HEADS * length),
        ),
        compiler_params=params,
        name="first",
    )(owner, prefix_len, tokens, w_uvqk, cache)
    weights = pl.pallas_call(
        functools.partial(weigh_kernel, head, scale),
        in_specs=[vmem] * (1 + pieces),
        out_specs=[vmem] * pieces,
        out_shape=[jax.ShapeDtypeStruct((HEADS, slots, length), jnp.bfloat16)] * pieces,
        cost_estimate=pl.CostEstimate(
            flops=2 * slots * width * length * pieces,
            bytes_accessed=2 * length * width * pieces,
            transcendentals=slots * HEADS * length * pieces,
        ),
        compiler_params=params,
        name="weigh",
    )(query, *keys)
    result = pl.pallas_call(
        functools.partial(last_kernel, head, pieces),
        in_specs=[smem] * 3 + [vmem] * (4 + 2 * pieces),
        out_specs=vmem,
        out_shape=rows(jnp.bfloat16),
        scratch_shapes=[pltpu.VMEM((slots, width), jnp.float32)],
        cost_estimate=pl.CostEstimate(
            flops=2 * slots * width * (width + length * pieces),
            bytes_accessed=2 * width * width + 2 * length * width * pieces,
            transcendentals=slots,
        ),
        compiler_params=params,
        name="last",
    )(owner, counts, prefix_len, acc, gate_u, norm_gain.reshape(1, width), w_output, *weights, *values)
    return result[None]


def solution(mesh):
    in_specs = (
        P("group", "helper", None),
        P("group", None, "helper", None),
        P(),
        P(),
        P(),
        P(),
        P(),
        P(),
    )
    out_specs = P("group", "helper", None)
    return jax.shard_map(local, mesh=mesh, in_specs=in_specs, out_specs=out_specs, check_vma=False)
```

```python
import functools
import math

import jax
import jax.numpy as jnp
from jax import lax
from jax.experimental import pallas as pl
from jax.experimental.pallas import tpu as pltpu
from jax.sharding import PartitionSpec as P

HEADS = 8
EPS = 1e-05


def silu(v):
    t = v * 0.5
    return t + t * jnp.tanh(t)


def weigh(query, keys, scale):
    scores = lax.dot_general(
        query, keys, (((1,), (1,)), ((), ())), preferred_element_type=jnp.float32
    )
    t = scores * (0.5 * scale)
    return (t + t * jnp.tanh(t)).astype(jnp.bfloat16)


def user_here(owner):
    groups = lax.axis_size("group")
    return lax.rem(lax.axis_index("group") - owner[0] + groups, groups)


def piece_base(away, length):
    helpers = lax.axis_size("helper")
    return lax.rem(lax.axis_index("helper") - away + helpers, helpers) * length


def seen(values, base, visible):
    rows = lax.broadcasted_iota(jnp.int32, values.shape, 0) + base
    return jnp.where(rows < visible, values, jnp.zeros_like(values))


def first_kernel(head, scale, owner, prefix_len, tok, w, cache, u_out, q_out, acc_out):
    width = tok.shape[1]
    wide = 2 * head
    length = cache.shape[1]
    visible = prefix_len[user_here(owner)]
    base = piece_base(0, length)
    for pair in range(width // wide):
        cols = slice(pair * wide, (pair + 1) * wide)

        def project(k):
            at = slice(k * width + pair * wide, k * width + (pair + 1) * wide)
            return silu(jnp.dot(tok[...], w[:, at], preferred_element_type=jnp.float32))

        query = project(2).astype(jnp.bfloat16)
        q_out[:, cols] = query
        own_k = project(3).astype(jnp.bfloat16).astype(jnp.float32)
        own_v = project(1).astype(jnp.bfloat16).astype(jnp.float32)
        u_out[:, cols] = project(0)
        prod = query.astype(jnp.float32) * own_k
        values = seen(cache[1, :, cols], base, visible)
        for n in range(wide // head):
            here = slice(n * head, (n + 1) * head)
            at = slice(pair * wide + n * head, pair * wide + (n + 1) * head)
            selfw = silu(jnp.sum(prod[:, here], axis=1, keepdims=True) * scale)
            selfw = selfw.astype(jnp.bfloat16).astype(jnp.float32)
            weights = weigh(query[:, here], cache[0, :, at], scale)
            mixed = jnp.dot(weights, values[:, here], preferred_element_type=jnp.float32)
            acc_out[:, at] = mixed + selfw * own_v[:, here]


def last_kernel(head, scale, pieces, owner, counts, prefix_len, q, acc, u, gain, w_out, *refs):
    caches, out, values, total, staged, sems = refs[:pieces], *refs[pieces:]
    slots, width = acc.shape
    length = caches[0].shape[1]
    user = user_here(owner)
    visible = prefix_len[user]
    live = counts[user] - lax.axis_index("helper") * slots
    for p in range(pieces):
        values[p] = seen(caches[p][1], piece_base(p + 1, length), visible)
    block = math.gcd(slots, 128)
    copies = []
    for first in range(0, slots, block):
        rows = slice(first, first + block)
        for n in range(width // head):
            at = slice(n * head, (n + 1) * head)
            mixed = acc[rows, at]
            for p in range(pieces):
                weights = weigh(q[rows, at], caches[p][0, :, at], scale)
                mixed += jnp.dot(weights, values[p, :, at], preferred_element_type=jnp.float32)
            total[rows, at] = mixed
        a = total[rows, :]
        centre = a - jnp.mean(a, axis=-1, keepdims=True)
        spread = jnp.mean(centre * centre, axis=-1, keepdims=True)
        normed = (centre * lax.rsqrt(spread + EPS) * gain[...] * u[rows, :]).astype(jnp.bfloat16)
        result = jnp.dot(normed, w_out[...], preferred_element_type=jnp.float32)
        places = lax.broadcasted_iota(jnp.int32, result.shape, 0) + first
        staged[rows, :] = jnp.where(places < live, result, 0.0).astype(jnp.bfloat16)
        copy = pltpu.make_async_copy(staged.at[rows], out.at[rows], sems.at[first // block])
        copy.start()
        copies.append(copy)
    for copy in copies:
        copy.wait()


def local(candidates, prefix_cache, w_uvqk, w_output, norm_gain, owner, counts, prefix_len):
    groups = lax.axis_size("group")
    helpers = lax.axis_size("helper")
    _, slots, width = candidates.shape
    length = prefix_cache.shape[2]
    head = width // HEADS
    scale = head ** (-0.5)
    cache = prefix_cache.reshape(2, length, width)
    pieces = helpers - 1

    def from_helper(value, away):
        pairs = [(i, (i + away) % helpers) for i in range(helpers)]
        return lax.ppermute(value, "helper", pairs)

    got = [from_helper(cache, away) for away in range(1, helpers)]

    def turn(s):
        pairs = [(i, (i + s) % groups) for i in range(groups)]
        return lambda t: lax.ppermute(t, "group", pairs)

    tokens = lax.switch(owner[0], [turn(s) for s in range(groups)], candidates[0])

    smem = pl.BlockSpec(memory_space=pltpu.SMEM)
    vmem = pl.BlockSpec(memory_space=pltpu.VMEM)
    params = pltpu.CompilerParams(vmem_limit_bytes=28 * 1024 * 1024)
    rows = lambda kind: jax.ShapeDtypeStruct((slots, width), kind)
    gate_u, query, acc = pl.pallas_call(
        functools.partial(first_kernel, head, scale),
        in_specs=[smem, smem, vmem, vmem, vmem],
        out_specs=[vmem] * 3,
        out_shape=[rows(jnp.float32), rows(jnp.bfloat16), rows(jnp.float32)],
        cost_estimate=pl.CostEstimate(
            flops=2 * slots * width * (4 * width + 2 * length),
            bytes_accessed=8 * width * width + 4 * length * width + 12 * slots * width,
            transcendentals=slots * (4 * width + HEADS * length),
        ),
        compiler_params=params,
        name="first",
    )(owner, prefix_len, tokens, w_uvqk, cache)
    result = pl.pallas_call(
        functools.partial(last_kernel, head, scale, pieces),
        in_specs=[smem] * 3 + [vmem] * (5 + pieces),
        out_specs=pl.BlockSpec(memory_space=pl.ANY),
        out_shape=rows(jnp.bfloat16),
        scratch_shapes=[
            pltpu.VMEM((pieces, length, width), jnp.bfloat16),
            pltpu.VMEM((slots, width), jnp.float32),
            pltpu.VMEM((slots, width), jnp.bfloat16),
            pltpu.SemaphoreType.DMA((slots // math.gcd(slots, 128),)),
        ],
        cost_estimate=pl.CostEstimate(
            flops=2 * slots * width * (width + 2 * length * pieces),
            bytes_accessed=2 * width * width + 4 * length * width * pieces,
            transcendentals=slots * HEADS * length * pieces,
        ),
        compiler_params=params,
        name="last",
    )(owner, counts, prefix_len, query, acc, gate_u, norm_gain.reshape(1, width), w_output, *got)
    return result[None]


def solution(mesh):
    in_specs = (
        P("group", "helper", None),
        P("group", None, "helper", None),
        P(),
        P(),
        P(),
        P(),
        P(),
        P(),
    )
    out_specs = P("group", "helper", None)
    return jax.shard_map(local, mesh=mesh, in_specs=in_specs, out_specs=out_specs, check_vma=False)
```

```python
import functools
import math

import jax
import jax.numpy as jnp
from jax import lax
from jax.experimental import pallas as pl
from jax.experimental.pallas import tpu as pltpu
from jax.sharding import PartitionSpec as P

HEADS = 8
EPS = 1e-05


def silu(v):
    t = v * 0.5
    return t + t * jnp.tanh(t)


def weigh(query, keys, scale):
    scores = lax.dot_general(
        query, keys, (((1,), (1,)), ((), ())), preferred_element_type=jnp.float32
    )
    t = scores * (0.5 * scale)
    return (t + t * jnp.tanh(t)).astype(jnp.bfloat16)


def user_here(owner):
    groups = lax.axis_size("group")
    return lax.rem(lax.axis_index("group") - owner[0] + groups, groups)


def piece_base(away, length):
    helpers = lax.axis_size("helper")
    return lax.rem(lax.axis_index("helper") - away + helpers, helpers) * length


def seen(values, base, visible):
    rows = lax.broadcasted_iota(jnp.int32, values.shape, 0) + base
    return jnp.where(rows < visible, values, jnp.zeros_like(values))


def first_kernel(
    head, scale, owner, prefix_len, tok, far, w, u_out, q_out, acc_out, cache, held, sems
):
    width = tok.shape[1]
    wide = 2 * head
    length = far.shape[1]
    visible = prefix_len[user_here(owner)]
    base = piece_base(0, length)
    copies = {}
    for pair in range(width // wide):
        for k in (2, 3, 1, 0):
            at = k * width + pair * wide
            spot = pair * 4 + k
            copy = pltpu.make_async_copy(w.at[:, at : at + wide], held.at[spot], sems.at[spot])
            copy.start()
            copies[spot] = copy
        if pair == 0:
            fetch = pltpu.make_async_copy(far, cache, sems.at[sems.shape[0] - 1])
            fetch.start()
    for pair in range(width // wide):
        cols = slice(pair * wide, (pair + 1) * wide)

        def project(k):
            copies[pair * 4 + k].wait()
            return silu(jnp.dot(tok[...], held[pair * 4 + k], preferred_element_type=jnp.float32))

        query = project(2).astype(jnp.bfloat16)
        q_out[:, cols] = query
        own_k = project(3).astype(jnp.bfloat16).astype(jnp.float32)
        own_v = project(1).astype(jnp.bfloat16).astype(jnp.float32)
        u_out[:, cols] = project(0)
        prod = query.astype(jnp.float32) * own_k
        if pair == 0:
            fetch.wait()
        values = seen(cache[1, :, cols], base, visible)
        for n in range(wide // head):
            here = slice(n * head, (n + 1) * head)
            at = slice(pair * wide + n * head, pair * wide + (n + 1) * head)
            selfw = silu(jnp.sum(prod[:, here], axis=1, keepdims=True) * scale)
            selfw = selfw.astype(jnp.bfloat16).astype(jnp.float32)
            weights = weigh(query[:, here], cache[0, :, at], scale)
            mixed = jnp.dot(weights, values[:, here], preferred_element_type=jnp.float32)
            acc_out[:, at] = mixed + selfw * own_v[:, here]


def last_kernel(head, scale, pieces, owner, counts, prefix_len, q, acc, u, gain, w_out, *refs):
    caches, out, total, staged, sems = refs[:pieces], *refs[pieces:]
    slots, width = acc.shape
    length = caches[0].shape[1]
    user = user_here(owner)
    visible = prefix_len[user]
    live = counts[user] - lax.axis_index("helper") * slots
    block = math.gcd(slots, 128)
    copies = []
    for n in range(width // head):
        at = slice(n * head, (n + 1) * head)
        mixed = acc[:, at]
        for p in range(pieces):
            weights = weigh(q[:, at], caches[p][0, :, at], scale)
            part = seen(caches[p][1, :, at], piece_base(p + 1, length), visible)
            mixed += jnp.dot(weights, part, preferred_element_type=jnp.float32)
        total[:, at] = mixed
    for first in range(0, slots, block):
        rows = slice(first, first + block)
        a = total[rows, :]
        centre = a - jnp.mean(a, axis=-1, keepdims=True)
        spread = jnp.mean(centre * centre, axis=-1, keepdims=True)
        normed = (centre * lax.rsqrt(spread + EPS) * gain[...] * u[rows, :]).astype(jnp.bfloat16)
        result = jnp.dot(normed, w_out[...], preferred_element_type=jnp.float32)
        places = lax.broadcasted_iota(jnp.int32, result.shape, 0) + first
        staged[rows, :] = jnp.where(places < live, result, 0.0).astype(jnp.bfloat16)
        copy = pltpu.make_async_copy(staged.at[rows], out.at[rows], sems.at[first // block])
        copy.start()
        copies.append(copy)
    for copy in copies:
        copy.wait()


def local(candidates, prefix_cache, w_uvqk, w_output, norm_gain, owner, counts, prefix_len):
    groups = lax.axis_size("group")
    helpers = lax.axis_size("helper")
    _, slots, width = candidates.shape
    length = prefix_cache.shape[2]
    head = width // HEADS
    scale = head ** (-0.5)
    cache = prefix_cache.reshape(2, length, width)
    pieces = helpers - 1

    def from_helper(value, away):
        pairs = [(i, (i + away) % helpers) for i in range(helpers)]
        return lax.ppermute(value, "helper", pairs)

    got = [from_helper(cache, away) for away in range(1, helpers)]

    def turn(s):
        pairs = [(i, (i + s) % groups) for i in range(groups)]
        return lambda t: lax.ppermute(t, "group", pairs)

    tokens = lax.switch(owner[0], [turn(s) for s in range(groups)], candidates[0])

    smem = pl.BlockSpec(memory_space=pltpu.SMEM)
    vmem = pl.BlockSpec(memory_space=pltpu.VMEM)
    hbm = pl.BlockSpec(memory_space=pltpu.HBM)
    params = pltpu.CompilerParams(vmem_limit_bytes=36 * 1024 * 1024)
    rows = lambda kind: jax.ShapeDtypeStruct((slots, width), kind)
    gate_u, query, acc = pl.pallas_call(
        functools.partial(first_kernel, head, scale),
        in_specs=[smem, smem, vmem, hbm, hbm],
        out_specs=[vmem] * 3,
        out_shape=[rows(jnp.float32), rows(jnp.bfloat16), rows(jnp.float32)],
        scratch_shapes=[
            pltpu.VMEM((2, length, width), jnp.bfloat16),
            pltpu.VMEM((4 * HEADS // 2, width, 2 * head), jnp.bfloat16),
            pltpu.SemaphoreType.DMA((4 * HEADS // 2 + 1,)),
        ],
        cost_estimate=pl.CostEstimate(
            flops=2 * slots * width * (4 * width + 2 * length),
            bytes_accessed=8 * width * width + 4 * length * width + 12 * slots * width,
            transcendentals=slots * (4 * width + HEADS * length),
        ),
        compiler_params=params,
        name="first",
    )(owner, prefix_len, tokens, cache, w_uvqk)
    result = pl.pallas_call(
        functools.partial(last_kernel, head, scale, pieces),
        in_specs=[smem] * 3 + [vmem] * (5 + pieces),
        out_specs=pl.BlockSpec(memory_space=pl.ANY),
        out_shape=rows(jnp.bfloat16),
        scratch_shapes=[
            pltpu.VMEM((slots, width), jnp.float32),
            pltpu.VMEM((slots, width), jnp.bfloat16),
            pltpu.SemaphoreType.DMA((slots // math.gcd(slots, 128),)),
        ],
        cost_estimate=pl.CostEstimate(
            flops=2 * slots * width * (width + 2 * length * pieces),
            bytes_accessed=2 * width * width + 4 * length * width * pieces,
            transcendentals=slots * HEADS * length * pieces,
        ),
        compiler_params=params,
        name="last",
    )(owner, counts, prefix_len, query, acc, gate_u, norm_gain.reshape(1, width), w_output, *got)
    return result[None]


def solution(mesh):
    in_specs = (
        P("group", "helper", None),
        P("group", None, "helper", None),
        P(),
        P(),
        P(),
        P(),
        P(),
        P(),
    )
    out_specs = P("group", "helper", None)
    return jax.shard_map(local, mesh=mesh, in_specs=in_specs, out_specs=out_specs, check_vma=False)
```

```python
import functools
import math

import jax
import jax.numpy as jnp
from jax import lax
from jax.experimental import pallas as pl
from jax.experimental.pallas import tpu as pltpu
from jax.sharding import PartitionSpec as P

HEADS = 8
EPS = 1e-05


def silu(v):
    t = v * 0.5
    return t + t * jnp.tanh(t)


def weigh(query, keys, scale):
    scores = lax.dot_general(
        query, keys, (((1,), (1,)), ((), ())), preferred_element_type=jnp.float32
    )
    t = scores * (0.5 * scale)
    return (t + t * jnp.tanh(t)).astype(jnp.bfloat16)


def user_here(owner):
    groups = lax.axis_size("group")
    return lax.rem(lax.axis_index("group") - owner[0] + groups, groups)


def piece_base(away, length):
    helpers = lax.axis_size("helper")
    return lax.rem(lax.axis_index("helper") - away + helpers, helpers) * length


def seen(values, base, visible):
    rows = lax.broadcasted_iota(jnp.int32, values.shape, 0) + base
    return jnp.where(rows < visible, values, jnp.zeros_like(values))


def first_kernel(head, scale, owner, prefix_len, tok, w, cache, u_out, q_out, acc_out):
    width = tok.shape[1]
    wide = 2 * head
    length = cache.shape[1]
    visible = prefix_len[user_here(owner)]
    base = piece_base(0, length)
    for pair in range(width // wide):
        cols = slice(pair * wide, (pair + 1) * wide)

        def project(k):
            at = slice(k * width + pair * wide, k * width + (pair + 1) * wide)
            return silu(jnp.dot(tok[...], w[:, at], preferred_element_type=jnp.float32))

        query = project(2).astype(jnp.bfloat16)
        q_out[:, cols] = query
        own_k = project(3).astype(jnp.bfloat16).astype(jnp.float32)
        own_v = project(1).astype(jnp.bfloat16).astype(jnp.float32)
        u_out[:, cols] = project(0)
        prod = query.astype(jnp.float32) * own_k
        values = seen(cache[1, :, cols], base, visible)
        for n in range(wide // head):
            here = slice(n * head, (n + 1) * head)
            at = slice(pair * wide + n * head, pair * wide + (n + 1) * head)
            selfw = silu(jnp.sum(prod[:, here], axis=1, keepdims=True) * scale)
            selfw = selfw.astype(jnp.bfloat16).astype(jnp.float32)
            weights = weigh(query[:, here], cache[0, :, at], scale)
            mixed = jnp.dot(weights, values[:, here], preferred_element_type=jnp.float32)
            acc_out[:, at] = mixed + selfw * own_v[:, here]


def last_kernel(head, scale, pieces, owner, counts, prefix_len, q, acc, u, gain, w_out, *refs):
    caches, out, total, staged, sems = refs[:pieces], *refs[pieces:]
    slots, width = acc.shape
    length = caches[0].shape[1]
    user = user_here(owner)
    visible = prefix_len[user]
    live = counts[user] - lax.axis_index("helper") * slots
    block = math.gcd(slots, 128)
    copies = []
    for n in range(width // head):
        at = slice(n * head, (n + 1) * head)
        mixed = acc[:, at]
        for p in range(pieces):
            weights = weigh(q[:, at], caches[p][0, :, at], scale)
            part = seen(caches[p][1, :, at], piece_base(p + 1, length), visible)
            mixed += jnp.dot(weights, part, preferred_element_type=jnp.float32)
        total[:, at] = mixed
    for first in range(0, slots, block):
        rows = slice(first, first + block)
        a = total[rows, :]
        centre = a - jnp.mean(a, axis=-1, keepdims=True)
        spread = jnp.mean(centre * centre, axis=-1, keepdims=True)
        normed = (centre * lax.rsqrt(spread + EPS) * gain[...] * u[rows, :]).astype(jnp.bfloat16)
        result = jnp.dot(normed, w_out[...], preferred_element_type=jnp.float32)
        places = lax.broadcasted_iota(jnp.int32, result.shape, 0) + first
        staged[rows, :] = jnp.where(places < live, result, 0.0).astype(jnp.bfloat16)
        copy = pltpu.make_async_copy(staged.at[rows], out.at[rows], sems.at[first // block])
        copy.start()
        copies.append(copy)
    for copy in copies:
        copy.wait()


def local(candidates, prefix_cache, w_uvqk, w_output, norm_gain, owner, counts, prefix_len):
    groups = lax.axis_size("group")
    helpers = lax.axis_size("helper")
    _, slots, width = candidates.shape
    length = prefix_cache.shape[2]
    head = width // HEADS
    scale = head ** (-0.5)
    cache = prefix_cache.reshape(2, length, width)
    pieces = helpers - 1

    def from_helper(value, away):
        pairs = [(i, (i + away) % helpers) for i in range(helpers)]
        return lax.ppermute(value, "helper", pairs)

    got = [from_helper(cache, away) for away in range(1, helpers)]

    def turn(s):
        pairs = [(i, (i + s) % groups) for i in range(groups)]
        return lambda t: lax.ppermute(t, "group", pairs)

    tokens = lax.switch(owner[0], [turn(s) for s in range(groups)], candidates[0])

    smem = pl.BlockSpec(memory_space=pltpu.SMEM)
    vmem = pl.BlockSpec(memory_space=pltpu.VMEM)
    params = pltpu.CompilerParams(vmem_limit_bytes=28 * 1024 * 1024)
    rows = lambda kind: jax.ShapeDtypeStruct((slots, width), kind)
    gate_u, query, acc = pl.pallas_call(
        functools.partial(first_kernel, head, scale),
        in_specs=[smem, smem, vmem, vmem, vmem],
        out_specs=[vmem] * 3,
        out_shape=[rows(jnp.float32), rows(jnp.bfloat16), rows(jnp.float32)],
        cost_estimate=pl.CostEstimate(
            flops=2 * slots * width * (4 * width + 2 * length),
            bytes_accessed=8 * width * width + 4 * length * width + 12 * slots * width,
            transcendentals=slots * (4 * width + HEADS * length),
        ),
        compiler_params=params,
        name="first",
    )(owner, prefix_len, tokens, w_uvqk, cache)
    result = pl.pallas_call(
        functools.partial(last_kernel, head, scale, pieces),
        in_specs=[smem] * 3 + [vmem] * (5 + pieces),
        out_specs=pl.BlockSpec(memory_space=pl.ANY),
        out_shape=rows(jnp.bfloat16),
        scratch_shapes=[
            pltpu.VMEM((slots, width), jnp.float32),
            pltpu.VMEM((slots, width), jnp.bfloat16),
            pltpu.SemaphoreType.DMA((slots // math.gcd(slots, 128),)),
        ],
        cost_estimate=pl.CostEstimate(
            flops=2 * slots * width * (width + 2 * length * pieces),
            bytes_accessed=2 * width * width + 4 * length * width * pieces,
            transcendentals=slots * HEADS * length * pieces,
        ),
        compiler_params=params,
        name="last",
    )(owner, counts, prefix_len, query, acc, gate_u, norm_gain.reshape(1, width), w_output, *got)
    return result[None]


def solution(mesh):
    in_specs = (
        P("group", "helper", None),
        P("group", None, "helper", None),
        P(),
        P(),
        P(),
        P(),
        P(),
        P(),
    )
    out_specs = P("group", "helper", None)
    return jax.shard_map(local, mesh=mesh, in_specs=in_specs, out_specs=out_specs, check_vma=False)
```
